32 devices in a mesh: row: 4 (over y, x), col: 8 (over z, core).
Axes of the slice: x: 2, y: 2, z: 4, core: 2. Of those that a mesh axis runs over, the one named last changes fastest.
Arguments:
- tokens: bfloat16 [4096, 2048], P(('row', 'col')), may hold values from -6 to 6
- norm_gain: float32 [2048], replicated, may hold values from 0.5 to 1.5
- router_weight: bfloat16 [2048, 16], P('row'), may hold values from -0.125 to 0.125
- expert_ids: int32 [4096, 3], P(('row', 'col')), may hold values from 0 to 15, all different within a row; in each aligned block of 128 rows (0 to 127, 128 to 255, ...) at most 32 rows name the same one
- w_gate: bfloat16 [32, 2048, 704], P(('row', 'col')), may hold values from -0.125 to 0.125
- w_up: bfloat16 [32, 2048, 704], P(('row', 'col')), may hold values from -0.125 to 0.125
- w_down: bfloat16 [32, 704, 2048], P(('row', 'col')), may hold values from -0.15625 to 0.15625
- grad_mixed: bfloat16 [4096, 2048], P(('row', 'col')), may hold values from -6 to 6
Outputs:
- mixed: bfloat16 [4096, 2048], P(('row', 'col'))
- grad_tokens: bfloat16 [4096, 2048], P(('row', 'col'))
- grad_gain: float32 [2048], replicated
- grad_router: float32 [2048, 16], P('row')
- grad_gate: bfloat16 [32, 2048, 704], P(('row', 'col'))
- grad_up: bfloat16 [32, 2048, 704], P(('row', 'col'))
- grad_down: bfloat16 [32, 704, 2048], P(('row', 'col'))
The draws below stay inside these ranges and needn't reach their ends.
Inputs may be any that keep to these rules, and one draw needn't show every extreme that they name: `expert_ids`: each row names 3 different experts; in each aligned block of 128 rows (the tokens of one device) no expert is named by more than 32 rows, a bound that some block reaches.
All inputs are finite; a program needn't handle non-finite values.
Results may differ from the reference program's by a relative error of at most 0.0083.
Values may be sent and summed in bfloat16 or wider, within the bound.
A program may use at most 128 MiB of HBM per device.

```python
import math
import jax
import jax.numpy as jnp
import numpy as np
from jax import lax

D = 2048
FF = 1408
TOP = 3
TOK_DEV = 128
EXPERTS = 16
HALF_FF = 704
HALVES = 32
CAP = 32
TOKENS = 4096
N_ROW = 4
N_COL = 8


def levels(own_key, dims, shards, smallest, top_value):
    def one(dim, shards_of):
        heights = jax.random.uniform(jax.random.fold_in(jax.random.fold_in(own_key, 6), dim), (shards_of,), jnp.float32, smallest / len(shards), top_value / len(shards))
        return jnp.repeat(jnp.exp(heights), dims[dim] // shards_of).reshape((-1,) + (1,) * (len(dims) - dim - 1))

    factor_of = one(*shards[0])
    for cut in shards[1:]:
        factor_of = factor_of * one(*cut)
    return factor_of


def deal_out(rng, own, number, rows, count, top, limit, slope):
    order = jax.random.permutation(rng, count)
    packed, common = portions_of(count, rows * top, limit, slope, True), portions_of(count, rows * top, limit, slope, False)
    places = jnp.arange(count)

    def named(sizes, turn):
        used = int((sizes > 0).sum())
        fixed = max(1, used // 4)
        shifted = fixed + (places - fixed + turn * (used - fixed)) % max(1, count - fixed)
        return jnp.zeros((count,), jnp.int32).at[order[jnp.where(places < fixed, places, shifted)]].set(jnp.asarray(sizes, jnp.int32))

    sizes = jnp.where(number % 4 == 0, named(packed, number // 4), named(common, number - number // 4 - 1))
    mixed = jax.random.permutation(jax.random.fold_in(own, 3), count)
    giver, receiver = mixed[0:count // 2 * 2:2], mixed[1:count // 2 * 2:2]
    room = jnp.minimum(sizes[giver] - 1, limit - sizes[receiver]) // 2
    room = jnp.where((giver == order[0]) | (receiver == order[0]) | (sizes[receiver] == 0), 0, jnp.maximum(room, 0))
    shifted = jax.random.randint(jax.random.fold_in(own, 4), (count // 2,), 0, 1 << 20) % (room + 1)
    sizes = sizes.at[giver].add(-shifted).at[receiver].add(shifted)
    labels = jnp.searchsorted(jnp.cumsum(sizes), jnp.arange(rows * top), side="right").astype(jnp.int32)
    listing = labels.reshape(top, rows).T
    listing = listing[jax.random.permutation(jax.random.fold_in(own, 1), rows)]
    turn = jax.random.randint(jax.random.fold_in(own, 2), (rows, 1), 0, top)
    return jnp.take_along_axis(listing, (jnp.arange(top)[None, :] + turn) % top, axis=1)


def portions_of(number_of, total, bound, slope, full):
    weights = [(1 << 20) // math.isqrt(standing ** slope) + 1 for standing in range(1, number_of + 1)]
    largest = bound if full else min(bound, max(-(-total // number_of), total * weights[0] // sum(weights)))
    least = 1 if total - largest >= number_of - 1 else 0
    counts, surplus = [largest] + [least] * (number_of - 1), total - largest - least * (number_of - 1)
    while surplus > 0:
        free = [i for i in range(1, number_of) if counts[i] < largest] or [i for i in range(1, number_of) if counts[i] < bound]
        whole, remaining = sum([weights[i] for i in free]), surplus
        for i in free:
            more = min(bound - counts[i], max(1, remaining * weights[i] // whole), surplus)
            counts[i] = counts[i] + more
            surplus = surplus - more
    return np.array(counts)


def normal_values(own_key, shape, scale, bound, split=(), held_as=jnp.bfloat16):
    values = jax.random.normal(own_key, shape, jnp.float32) * scale
    if len(split) > 0:
        values = levels(own_key, shape, split, -0.22, 0.18) * values
    return jnp.clip(values, min=-bound, max=bound).astype(held_as)


def setup_inputs(seed: int = 0) -> dict:
    splits = jax.random.split(jax.random.key(seed), 9)
    tokens = normal_values(splits[0], (TOKENS, D), 1.0, 6.0, ((0, 32),))
    norm_gain = jnp.clip(jax.random.uniform(splits[1], (D,), jnp.float32, 0.5, 1.5), 0.5, 1.5)
    router_weight = normal_values(splits[2], (D, EXPERTS), D ** -0.5, 0.125, ((0, 4),))
    expert_ids_keys = jax.random.split(jax.random.fold_in(splits[3], 1), TOKENS // TOK_DEV)
    expert_ids_turns = jax.random.permutation(jax.random.fold_in(splits[3], 3), TOKENS // TOK_DEV)
    expert_ids = jax.vmap(lambda own, number: deal_out(jax.random.fold_in(splits[3], 2), own, number, TOK_DEV, EXPERTS, TOP, CAP, 1))(expert_ids_keys, expert_ids_turns).reshape((TOKENS, TOP))
    w_gate = normal_values(splits[4], (HALVES, D, HALF_FF), D ** -0.5, 0.125, ((0, 32),))
    w_up = normal_values(splits[5], (HALVES, D, HALF_FF), D ** -0.5, 0.125, ((0, 32),))
    w_down = normal_values(splits[6], (HALVES, HALF_FF, D), FF ** -0.5, 0.15625, ((0, 32),))
    grad_mixed = normal_values(splits[7], (TOKENS, D), 1.0, 6.0, ((0, 32),))
    return {"tokens": tokens, "norm_gain": norm_gain, "router_weight": router_weight, "expert_ids": expert_ids, "w_gate": w_gate, "w_up": w_up, "w_down": w_down, "grad_mixed": grad_mixed}


epsilon = 1e-06

def half_pass(slot_rows, grad_out, w_gate, w_up, w_down):
    gate_pre = jnp.dot(slot_rows, w_gate, preferred_element_type=jnp.float32)
    up_pre = jnp.dot(slot_rows, w_up, preferred_element_type=jnp.float32)
    sigmoid = jax.nn.sigmoid(gate_pre)
    swish_act = gate_pre * sigmoid
    hidden = (swish_act * up_pre).astype(jnp.bfloat16)
    partial_value = jnp.dot(hidden, w_down, preferred_element_type=jnp.float32).astype(jnp.bfloat16)
    d_hidden = lax.dot_general(grad_out, w_down, (((1,), (1,)), ((), ())), preferred_element_type=jnp.float32)
    d_gate = (d_hidden * up_pre * sigmoid * (1.0 + gate_pre * (1.0 - sigmoid))).astype(jnp.bfloat16)
    d_up = (d_hidden * swish_act).astype(jnp.bfloat16)
    backward = lax.dot_general(d_gate, w_gate, (((1,), (1,)), ((), ())), preferred_element_type=jnp.float32)
    backward = backward + lax.dot_general(d_up, w_up, (((1,), (1,)), ((), ())), preferred_element_type=jnp.float32)
    grad_rows = backward.astype(jnp.bfloat16)
    grad_wgate = lax.dot_general(slot_rows, d_gate, (((0,), (0,)), ((), ())), preferred_element_type=jnp.float32).astype(jnp.bfloat16)
    grad_wup = lax.dot_general(slot_rows, d_up, (((0,), (0,)), ((), ())), preferred_element_type=jnp.float32).astype(jnp.bfloat16)
    grad_wdown = lax.dot_general(hidden, grad_out, (((0,), (0,)), ((), ())), preferred_element_type=jnp.float32).astype(jnp.bfloat16)
    return (partial_value, grad_rows, grad_wgate, grad_wup, grad_wdown)

def slot_places(expert_ids):
    blocks = N_ROW * N_COL
    flat_ids = expert_ids.reshape(blocks, TOK_DEV * TOP)
    onehot = (flat_ids[:, :, None] == jnp.arange(EXPERTS, dtype=jnp.int32)[None, None, :]).astype(jnp.int32)
    earlier = jnp.cumsum(onehot, axis=1, dtype=jnp.int32) - onehot
    ranks = lax.optimization_barrier(jnp.sum(earlier * onehot, axis=2, dtype=jnp.int32))
    block_ids = jnp.arange(blocks, dtype=jnp.int32)[:, None]
    return (flat_ids * (blocks * CAP) + block_ids * CAP + ranks).reshape(-1).astype(jnp.int32)

def reference(tokens, norm_gain, router_weight, expert_ids, w_gate, w_up, w_down, grad_mixed):
    blocks = N_ROW * N_COL
    tokens_f = tokens.astype(jnp.float32)
    inverse = lax.rsqrt(lax.optimization_barrier(jnp.mean(tokens_f * tokens_f, axis=1, keepdims=True)) + epsilon)
    normed = tokens_f * inverse
    scaled = (normed * norm_gain).astype(jnp.bfloat16)
    logits = jnp.dot(scaled, router_weight, preferred_element_type=jnp.float32)
    scores = jax.nn.sigmoid(logits)
    chosen = (expert_ids[:, :, None] == jnp.arange(EXPERTS, dtype=jnp.int32)[None, None, :]).astype(jnp.float32)
    gate_vals = lax.optimization_barrier(jnp.sum(chosen * scores[:, None, :], axis=2))
    upstream = grad_mixed.astype(jnp.float32)
    slot_grads = (gate_vals[:, :, None] * upstream[:, None, :]).astype(jnp.bfloat16).reshape(-1, D)
    places = slot_places(expert_ids)
    slot_inputs = jnp.repeat(scaled, TOP, axis=0)
    total_rows = EXPERTS * blocks * CAP
    buffer_in = jnp.zeros((total_rows, D), jnp.bfloat16).at[places].set(slot_inputs).reshape(EXPERTS, blocks * CAP, D)
    buffer_grad = jnp.zeros((total_rows, D), jnp.bfloat16).at[places].set(slot_grads).reshape(EXPERTS, blocks * CAP, D)
    gate_halves = w_gate.reshape(EXPERTS, 2, D, HALF_FF)
    up_halves = w_up.reshape(EXPERTS, 2, D, HALF_FF)
    down_halves = w_down.reshape(EXPERTS, 2, HALF_FF, D)

    def per_expert(items):
        slot_rows, grad_out, gate_pair, up_pair, down_pair = items
        first = half_pass(slot_rows, grad_out, gate_pair[0], up_pair[0], down_pair[0])
        second = half_pass(slot_rows, grad_out, gate_pair[1], up_pair[1], down_pair[1])
        outputs = (first[0].astype(jnp.float32) + second[0].astype(jnp.float32)).astype(jnp.bfloat16)
        grad_rows = (first[1].astype(jnp.float32) + second[1].astype(jnp.float32)).astype(jnp.bfloat16)
        return (outputs, grad_rows, jnp.stack([first[2], second[2]]), jnp.stack([first[3], second[3]]), jnp.stack([first[4], second[4]]))
    expert_out, expert_grad, grad_gate, grad_up, grad_down = lax.map(per_expert, (buffer_in, buffer_grad, gate_halves, up_halves, down_halves))
    slot_out = expert_out.reshape(total_rows, D)[places].reshape(-1, TOP, D).astype(jnp.float32)
    slot_back = expert_grad.reshape(total_rows, D)[places].reshape(-1, TOP, D).astype(jnp.float32)
    mixed = (tokens_f + lax.optimization_barrier(jnp.sum(gate_vals[:, :, None] * slot_out, axis=1))).astype(jnp.bfloat16)
    grad_gates = lax.optimization_barrier(jnp.sum(slot_out * upstream[:, None, :], axis=2))
    grad_logits = (lax.optimization_barrier(jnp.sum(chosen * grad_gates[:, :, None], axis=1)) * scores * (1.0 - scores)).astype(jnp.bfloat16)
    grad_scaled = lax.optimization_barrier(jnp.sum(slot_back, axis=1)) + lax.dot_general(grad_logits, router_weight, (((1,), (1,)), ((), ())), preferred_element_type=jnp.float32)
    grad_router = lax.dot_general(scaled, grad_logits, (((0,), (0,)), ((), ())), preferred_element_type=jnp.float32)
    grad_gain = lax.optimization_barrier(jnp.sum(grad_scaled * normed, axis=0))
    grad_normed = grad_scaled * norm_gain
    grad_tokens = (upstream + inverse * (grad_normed - normed * lax.optimization_barrier(jnp.mean(grad_normed * normed, axis=1, keepdims=True)))).astype(jnp.bfloat16)
    return (mixed, grad_tokens, grad_gain, grad_router, grad_gate.reshape(2 * EXPERTS, D, HALF_FF), grad_up.reshape(2 * EXPERTS, D, HALF_FF), grad_down.reshape(2 * EXPERTS, HALF_FF, D))
```

```python
import functools
import jax
import jax.numpy as jnp
from jax import lax
from jax.experimental import pallas as pl
from jax.experimental.pallas import tpu as pltpu
from jax.sharding import PartitionSpec as P

epsilon = 1e-06
bf16, f32 = jnp.bfloat16, jnp.float32
NT = (((1,), (1,)), ((), ()))
TN = (((0,), (0,)), ((), ()))


def mm(a, b, dims=(((1,), (0,)), ((), ()))):
    return lax.dot_general(a, b, dims, preferred_element_type=f32)


def swapped(block, axis, apart):
    count = lax.axis_size(axis)
    route = []
    for low in range(count):
        high = low | 1 << apart
        if high != low and high < count:
            route += [(low, high), (high, low)]
    return lax.ppermute(block, axis, route)


def half_pass(slot_rows, grad_out, w_gate, w_up, w_down):
    gate_pre = jnp.dot(slot_rows, w_gate, preferred_element_type=jnp.float32)
    up_pre = jnp.dot(slot_rows, w_up, preferred_element_type=jnp.float32)
    sigmoid = jax.nn.sigmoid(gate_pre)
    swish_act = gate_pre * sigmoid
    hidden = (swish_act * up_pre).astype(jnp.bfloat16)
    partial_value = jnp.dot(hidden, w_down, preferred_element_type=jnp.float32).astype(jnp.bfloat16)
    d_hidden = lax.dot_general(
        grad_out, w_down, (((1,), (1,)), ((), ())), preferred_element_type=jnp.float32
    )
    d_gate = (d_hidden * up_pre * sigmoid * (1.0 + gate_pre * (1.0 - sigmoid))).astype(jnp.bfloat16)
    d_up = (d_hidden * swish_act).astype(jnp.bfloat16)
    backward = lax.dot_general(
        d_gate, w_gate, (((1,), (1,)), ((), ())), preferred_element_type=jnp.float32
    )
    backward = backward + lax.dot_general(
        d_up, w_up, (((1,), (1,)), ((), ())), preferred_element_type=jnp.float32
    )
    grad_rows = backward.astype(jnp.bfloat16)
    grad_wgate = lax.dot_general(
        slot_rows, d_gate, (((0,), (0,)), ((), ())), preferred_element_type=jnp.float32
    ).astype(jnp.bfloat16)
    grad_wup = lax.dot_general(
        slot_rows, d_up, (((0,), (0,)), ((), ())), preferred_element_type=jnp.float32
    ).astype(jnp.bfloat16)
    grad_wdown = lax.dot_general(
        hidden, grad_out, (((0,), (0,)), ((), ())), preferred_element_type=jnp.float32
    ).astype(jnp.bfloat16)
    return (partial_value, grad_rows, grad_wgate, grad_wup, grad_wdown)


def to_experts(buffer, capacity):
    width = buffer.shape[1]
    halves = 2 * (buffer.shape[0] // capacity)
    pieces = buffer.reshape(halves, capacity // 2, width)
    mine = lax.all_to_all(pieces, ("row", "col"), split_axis=0, concat_axis=0, tiled=True)
    other = swapped(mine, "col", 0)
    arrived = jnp.concatenate([mine, other], axis=0).reshape(-1, width)
    return arrived


def from_experts(partial_value, capacity):
    width = partial_value.shape[1]
    halves = partial_value.shape[0] // capacity
    sections = partial_value.reshape(2, halves, capacity // 2, width)
    returned = swapped(sections[1], "col", 0)
    summed = (sections[0].astype(jnp.float32) + returned.astype(jnp.float32)).astype(jnp.bfloat16)
    result = lax.all_to_all(
        summed, ("row", "col"), split_axis=0, concat_axis=0, tiled=True
    ).reshape(-1, width)
    return result


def wide_local(tokens, norm_gain, router_weight, expert_ids, w_gate, w_up, w_down, grad_mixed):
    tok_count, width = tokens.shape
    top_count = expert_ids.shape[1]
    experts_all = router_weight.shape[1]
    capacity = 2 * ((2 * tok_count * top_count + 3 * experts_all - 1) // (3 * experts_all))
    tokens_f = tokens.astype(jnp.float32)
    inverse = lax.rsqrt(jnp.mean(tokens_f * tokens_f, axis=1, keepdims=True) + epsilon)
    normed = tokens_f * inverse
    scaled = (normed * norm_gain).astype(jnp.bfloat16)
    logits = jnp.dot(
        scaled,
        lax.all_gather(router_weight, "row", axis=0, tiled=True),
        preferred_element_type=jnp.float32,
    )
    scores = jax.nn.sigmoid(logits)
    expert_range = jnp.arange(experts_all, dtype=jnp.int32)
    chosen = (expert_ids[:, :, None] == expert_range[None, None, :]).astype(jnp.float32)
    gate_vals = jnp.sum(chosen * scores[:, None, :], axis=2)
    upstream = grad_mixed.astype(jnp.float32)
    slot_grads = (
        (gate_vals[:, :, None] * upstream[:, None, :]).astype(jnp.bfloat16).reshape(-1, width)
    )
    flat_ids = expert_ids.reshape(-1)
    onehot = (flat_ids[:, None] == expert_range[None, :]).astype(jnp.int32)
    ranks = jnp.sum(
        (jnp.cumsum(onehot, axis=0, dtype=jnp.int32) - onehot) * onehot, axis=1, dtype=jnp.int32
    )
    rotation = lax.axis_index("col") % 2 * (capacity // 2)
    places = flat_ids * capacity + (ranks + rotation) % capacity
    send_in = (
        jnp.zeros((experts_all * capacity, width), jnp.bfloat16)
        .at[places]
        .set(jnp.repeat(scaled, top_count, axis=0))
    )
    send_grad = jnp.zeros((experts_all * capacity, width), jnp.bfloat16).at[places].set(slot_grads)
    rows_in = to_experts(send_in, capacity)
    rows_grad = to_experts(send_grad, capacity)
    partial_value, grad_rows, grad_wgate, grad_wup, grad_wdown = half_pass(
        rows_in, rows_grad, w_gate[0], w_up[0], w_down[0]
    )
    slot_out = (
        from_experts(partial_value, capacity)[places]
        .reshape(tok_count, top_count, width)
        .astype(jnp.float32)
    )
    slot_back = (
        from_experts(grad_rows, capacity)[places]
        .reshape(tok_count, top_count, width)
        .astype(jnp.float32)
    )
    mixed = (tokens_f + jnp.sum(gate_vals[:, :, None] * slot_out, axis=1)).astype(jnp.bfloat16)
    grad_gates = jnp.sum(slot_out * upstream[:, None, :], axis=2)
    grad_logits = (
        jnp.sum(chosen * grad_gates[:, :, None], axis=1) * scores * (1.0 - scores)
    ).astype(jnp.bfloat16)
    grad_scaled = jnp.sum(slot_back, axis=1) + lax.dot_general(
        grad_logits,
        lax.all_gather(router_weight, "row", axis=0, tiled=True),
        (((1,), (1,)), ((), ())),
        preferred_element_type=jnp.float32,
    )
    router_terms = lax.dot_general(
        scaled, grad_logits, (((0,), (0,)), ((), ())), preferred_element_type=jnp.float32
    )
    gain_terms = jnp.sum(grad_scaled * normed, axis=0)
    router_shard = lax.psum_scatter(router_terms, "row", scatter_dimension=0, tiled=True)
    grad_router = lax.psum(router_shard, "col")
    grad_gain = lax.psum(gain_terms, ("row", "col"))
    grad_normed = grad_scaled * norm_gain
    grad_tokens = (
        upstream
        + inverse * (grad_normed - normed * jnp.mean(grad_normed * normed, axis=1, keepdims=True))
    ).astype(jnp.bfloat16)
    return (
        mixed,
        grad_tokens,
        grad_gain,
        grad_router,
        grad_wgate[None],
        grad_wup[None],
        grad_wdown[None],
    )


def exchange(
    rows, lines, cap,
    scaled, gm, pos_in, rt_in, wg_hbm, wu_hbm, wd_hbm,
    acc, gg_out, meta, rt, x_out, hid_out, dg_out, du_out,
    wg, wu, wd, zin, zmeta, sbuf, xb, hid, dgb, dub, po, pr, yb, ps, cr, ggs,
    zsend, zrecv, msend, mrecv, psend, precv, csend, crecv, bsend, brecv,
    ysend, yrecv, hsend, hrecv, gsend, grecv, wsem, osem, rsend, rrecv,
):
    r = lax.axis_index("row")
    c = lax.axis_index("col")
    z = c // 2
    core = c % 2
    tok, width = scaled.shape
    slots = rows * cap
    n = lines
    short = jnp.minimum(z, n - 1 - z)
    up_long = z < n - 1 - z

    def chunk(i):
        near = jnp.where(i % 2 == 1, z + (i + 1) // 2, z - (i + 1) // 2)
        far = jnp.where(up_long, z + i - short, z - i + short)
        return jnp.where(i <= 2 * short, near, far)

    def dev(row, line, cr_):
        return {"row": row, "col": line * 2 + cr_}

    def rdma(src, dst, ss, rs, where):
        return pltpu.make_async_remote_copy(
            src_ref=src, dst_ref=dst, send_sem=ss, recv_sem=rs, device_id=where,
            device_id_type=pl.DeviceIdType.MESH,
        )

    def zcopy(a, zb, d, own):
        src = (gm if a else scaled) if own else zin.at[a, zb]
        line = z + 1 if d == 0 else z - 1
        return rdma(src, zin.at[a, zb], zsend.at[a, d, zb], zrecv.at[a, zb], dev(r, line, core))

    def mcopy(zb, d, own):
        line = z + 1 if d == 0 else z - 1
        return rdma(meta if own else zmeta.at[zb], zmeta.at[zb], msend.at[d, zb], mrecv.at[zb],
                    dev(r, line, core))

    def pcopy(a, zb, r2):
        return rdma(sbuf.at[zb, r2], xb.at[a, zb, core, r], psend.at[a, zb, r2],
                    precv.at[a, zb, r], dev(r2, z, core))

    def ccopy(a, zb):
        return rdma(xb.at[a, zb, core], xb.at[a, zb, core], csend.at[a, zb], crecv.at[a, zb],
                    dev(r, z, 1 - core))

    def bcopy(a, zb):
        return rdma(po.at[a, zb, 1 - core], pr.at[zb], bsend.at[a, zb], brecv.at[a, zb],
                    dev(r, z, 1 - core))

    def ycopy(a, zb, r2):
        return rdma(po.at[a, zb, core, r2], yb.at[a, zb, r], ysend.at[a, zb, r2],
                    yrecv.at[a, zb, r], dev(r2, z, core))

    def hcopy(a, zb):
        nxt = jnp.where(zb > z, z + 1, z - 1)
        slot = jnp.where((nxt == zb) & (zb < z), n, zb)
        return rdma(ps.at[a, zb], cr.at[a, slot], hsend.at[a, zb], hrecv.at[a, slot],
                    dev(r, nxt, core))

    def gcopy(zb):
        return rdma(ggs.at[zb], gg_out.at[z], gsend.at[zb], grecv.at[z], dev(r, zb, core))

    def ocopies(zb):
        return [
            pltpu.make_async_copy(xb.at[0, zb], x_out.at[0, zb], osem.at[0, zb]),
            pltpu.make_async_copy(xb.at[1, zb], x_out.at[1, zb], osem.at[1, zb]),
            pltpu.make_async_copy(hid.at[zb], hid_out.at[zb], osem.at[2, zb]),
            pltpu.make_async_copy(dgb.at[zb], dg_out.at[zb], osem.at[3, zb]),
            pltpu.make_async_copy(dub.at[zb], du_out.at[zb], osem.at[4, zb]),
        ]

    wcopies = [
        pltpu.make_async_copy(wg_hbm, wg, wsem.at[0]),
        pltpu.make_async_copy(wu_hbm, wu, wsem.at[1]),
        pltpu.make_async_copy(wd_hbm, wd, wsem.at[2]),
    ]

    barrier = pltpu.get_barrier_semaphore()
    for o in range(1, rows):
        pl.semaphore_signal(barrier, inc=1, device_id=dev((r + o) % rows, z, core),
                            device_id_type=pl.DeviceIdType.MESH)
    for o in range(1, n):
        pl.semaphore_signal(barrier, inc=1, device_id=dev(r, (z + o) % n, core),
                            device_id_type=pl.DeviceIdType.MESH)
    pl.semaphore_signal(barrier, inc=1, device_id=dev(r, z, 1 - core),
                        device_id_type=pl.DeviceIdType.MESH)
    for w in wcopies:
        w.start()
    pl.semaphore_wait(barrier, rows + n - 1)

    has_up, has_down = z < n - 1, z > 0

    def own_sends(a):
        @pl.when(has_up)
        def _():
            zcopy(a, z, 0, True).start()

        @pl.when(has_down)
        def _():
            zcopy(a, z, 1, True).start()

    def meta_sends():
        @pl.when(has_up)
        def _():
            mcopy(z, 0, True).start()

        @pl.when(has_down)
        def _():
            mcopy(z, 1, True).start()

    def rcopy(r2):
        return rdma(rt_in, rt.at[r], rsend.at[r2], rrecv.at[r], dev(r2, z, core))

    for o in range(1, rows):
        rcopy((r + o) % rows).start()
    own_sends(0)
    rt[r] = rt_in[...]
    zin[0, z] = scaled[...]
    zin[1, z] = gm[...]
    for o in range(1, rows):
        r2 = (r + o) % rows
        rdma(rt_in, rt.at[r2], rsend.at[r2], rrecv.at[r2], dev(r2, z, core)).wait_recv()
    part = width // rows
    logits = mm(rt[0], scaled[:, :part], NT)
    for k in range(1, rows):
        logits = logits + mm(rt[k], scaled[:, k * part:(k + 1) * part], NT)
    scores = jax.nn.sigmoid(logits)
    for e in range(rows * lines):
        row, line = e // lines, e % lines
        meta[line, 0, row:row + 1, :] = pos_in[e:e + 1, :]
        meta[line, 1, row:row + 1, :] = scores[e:e + 1, :]
    zmeta[z] = meta[...]
    meta_sends()

    def onehot(zb):
        pos = zmeta[zb, z, 0]
        place = lax.broadcasted_iota(jnp.int32, (rows, cap, tok), 1).astype(f32)
        return jnp.where(pos[:, None, :] == place, 1.0, 0.0)

    def gates(zb, oh3):
        sc = zmeta[zb, z, 1]
        return jnp.sum(oh3 * sc[:, None, :], axis=2, keepdims=True).reshape(slots, 1)

    def each_row(fn):
        for o in range(1, rows):
            fn((r + o) % rows)

    def arrive(a, i):
        zb = chunk(i)

        @pl.when(i > 0)
        def _():
            zcopy(a, zb, 0, False).wait_recv()
            if a == 0:
                mcopy(zb, 0, False).wait_recv()

            @pl.when((zb < z) & has_up)
            def _():
                if a == 0:
                    mcopy(zb, 0, False).start()
                zcopy(a, zb, 0, False).start()

            @pl.when((zb > z) & has_down)
            def _():
                if a == 0:
                    mcopy(zb, 1, False).start()
                zcopy(a, zb, 1, False).start()

        oh3 = onehot(zb)
        oh = oh3.reshape(slots, tok).astype(bf16)
        got = mm(oh, zin[a, zb])
        if a == 1:
            got = got * gates(zb, oh3)
        got = got.astype(bf16).reshape(rows, cap, width)
        if a == 1:
            each_row(lambda r2: pcopy(0, zb, r2).wait_send())
        sbuf[zb] = got
        each_row(lambda r2: pcopy(a, zb, r2).start())
        xb[a, zb, core, r] = sbuf[zb, r]

    def process(a, i):
        zb = chunk(i)

        def got_row(r2):
            rdma(sbuf.at[zb, r2], xb.at[a, zb, core, r2], psend.at[a, zb, r2],
                 precv.at[a, zb, r2], dev(r2, z, core)).wait_recv()

        each_row(got_row)
        ccopy(a, zb).start()
        rdma(xb.at[a, zb, 1 - core], xb.at[a, zb, 1 - core], csend.at[a, zb], crecv.at[a, zb],
             dev(r, z, 1 - core)).wait_recv()
        x = xb[a, zb].reshape(2 * slots, width)
        if a == 0:
            @pl.when(i == 0)
            def _():
                for w in wcopies:
                    w.wait()

            g = mm(x, wg[...], NT)
            u = mm(x, wu[...], NT)
            s = jax.nn.sigmoid(g)
            sw = g * s
            h = (sw * u).astype(bf16)
            hid[zb] = h
            dub[zb] = sw.astype(bf16)
            dgb[zb] = (u * s * (1.0 + g * (1.0 - s))).astype(bf16)
            out = mm(h, wd[...])
        else:
            dh = mm(x, wd[...], NT)
            dg = (dh * dgb[zb].astype(f32)).astype(bf16)
            du = (dh * dub[zb].astype(f32)).astype(bf16)
            dgb[zb] = dg
            dub[zb] = du
            out = mm(dg, wg[...]) + mm(du, wu[...])
        po[a, zb] = out.astype(bf16).reshape(2, rows, cap, width)
        bcopy(a, zb).start()
        if a == 1:
            for o in ocopies(zb):
                o.start()
        bcopy(a, zb).wait_recv()
        po[a, zb, core] = (po[a, zb, core].astype(f32) + pr[zb].astype(f32)).astype(bf16)
        each_row(lambda r2: ycopy(a, zb, r2).start())
        yb[a, zb, r] = po[a, zb, core, r]

    def reduce(a, i):
        zb = chunk(i)

        def got_row(r2):
            rdma(po.at[a, zb, core, r2], yb.at[a, zb, r2], ysend.at[a, zb, r2],
                 yrecv.at[a, zb, r2], dev(r2, z, core)).wait_recv()

        each_row(got_row)
        oh3 = onehot(zb)
        oh2 = oh3.reshape(slots, tok)
        oh = oh2.astype(bf16)
        oht = oh2.T.astype(bf16)
        y = yb[a, zb].reshape(slots, width)
        if a == 0:
            y = (y.astype(f32) * gates(zb, oh3)).astype(bf16)
        total = mm(oht, y)

        @pl.when(i == 0)
        def _():
            acc[a] = total

        @pl.when(i > 0)
        def _():
            ps[a, zb] = total.astype(bf16)

        if a == 1:
            gmr = mm(oh, zin[1, zb])
            v = jnp.sum(gmr * yb[0, zb].reshape(slots, width).astype(f32), axis=1, keepdims=True)
            gg = jnp.sum(oh3 * v.reshape(rows, cap, 1), axis=1)

            @pl.when(i == 0)
            def _():
                gg_out[z] = gg

            @pl.when(i > 0)
            def _():
                ggs[zb] = gg
                gcopy(zb).start()

    def chain(a, i):
        zb = chunk(i)
        behind = jnp.where(zb > z, has_down, has_up)

        @pl.when(behind)
        def _():
            rdma(ps.at[a, zb], cr.at[a, zb], hsend.at[a, zb], hrecv.at[a, zb],
                 dev(r, z, 1 - core)).wait_recv()
            ps[a, zb] = (ps[a, zb].astype(f32) + cr[a, zb].astype(f32)).astype(bf16)

        hcopy(a, zb).start()

    def step(j, _):
        for a in range(2):
            @pl.when((j >= a * n) & (j < a * n + n))
            def _(a=a):
                arrive(a, j - a * n)

        @pl.when(j == 1)
        def _():
            own_sends(1)

        for a in range(2):
            @pl.when((j >= a * n + 1) & (j < a * n + n + 1))
            def _(a=a):
                process(a, j - a * n - 1)

        for a in range(2):
            @pl.when((j >= a * n + 2) & (j < a * n + n + 2))
            def _(a=a):
                reduce(a, j - a * n - 2)

        for a in range(2):
            first = a * n + n + 2

            @pl.when((j >= first) & (j < first + n - 1))
            def _(a=a, first=first):
                chain(a, n - 1 - (j - first))

        return 0

    lax.fori_loop(0, 3 * n + 1, step, 0)

    for a in range(2):
        @pl.when(has_down)
        def _(a=a):
            rdma(ps.at[a, z], cr.at[a, z], hsend.at[a, z], hrecv.at[a, z],
                 dev(r, z, 1 - core)).wait_recv()
            acc[a] = acc[a] + cr[a, z].astype(f32)

        @pl.when(has_up)
        def _(a=a):
            rdma(ps.at[a, z], cr.at[a, n], hsend.at[a, z], hrecv.at[a, n],
                 dev(r, z, 1 - core)).wait_recv()
            acc[a] = acc[a] + cr[a, n].astype(f32)

    each_row(lambda r2: rcopy(r2).wait_send())

    def finish(i, _):
        zb = chunk(i)
        for a in range(2):
            if a == 1:
                each_row(lambda r2: pcopy(a, zb, r2).wait_send())
            each_row(lambda r2: ycopy(a, zb, r2).wait_send())
            ccopy(a, zb).wait_send()
            bcopy(a, zb).wait_send()
        for o in ocopies(zb):
            o.wait()

        @pl.when(i == 0)
        def _():
            @pl.when(has_up)
            def _():
                mcopy(z, 0, True).wait_send()
                for a in range(2):
                    zcopy(a, z, 0, True).wait_send()

            @pl.when(has_down)
            def _():
                mcopy(z, 1, True).wait_send()
                for a in range(2):
                    zcopy(a, z, 1, True).wait_send()

        @pl.when(i > 0)
        def _():
            @pl.when((zb < z) & has_up)
            def _():
                mcopy(zb, 0, False).wait_send()
                for a in range(2):
                    zcopy(a, zb, 0, False).wait_send()

            @pl.when((zb > z) & has_down)
            def _():
                mcopy(zb, 1, False).wait_send()
                for a in range(2):
                    zcopy(a, zb, 1, False).wait_send()

            for a in range(2):
                hcopy(a, zb).wait_send()
            gcopy(zb).wait_send()
            rdma(ggs.at[zb], gg_out.at[zb], gsend.at[zb], grecv.at[zb],
                 dev(r, zb, core)).wait_recv()

        return 0

    lax.fori_loop(0, n, finish, 0)


def run_exchange(scaled, gm, pos, rt, wgt, wut, wd, rows, lines, cap):
    tok, width = scaled.shape
    half = wd.shape[0]
    slots = rows * cap
    m = 2 * slots
    DMA = pltpu.SemaphoreType.DMA
    V = pltpu.VMEM
    vm = pl.BlockSpec(memory_space=pltpu.VMEM)
    anyb = pl.BlockSpec(memory_space=pl.ANY)
    return pl.pallas_call(
        functools.partial(exchange, rows, lines, cap),
        out_shape=(
            jax.ShapeDtypeStruct((2, tok, width), f32),
            jax.ShapeDtypeStruct((lines, rows, tok), f32),
            jax.ShapeDtypeStruct((lines, 2, rows, tok), f32),
            jax.ShapeDtypeStruct((rows,) + rt.shape, bf16),
            jax.ShapeDtypeStruct((2, lines, 2, rows, cap, width), bf16),
            jax.ShapeDtypeStruct((lines, m, half), bf16),
            jax.ShapeDtypeStruct((lines, m, half), bf16),
            jax.ShapeDtypeStruct((lines, m, half), bf16),
        ),
        in_specs=[vm, vm, vm, vm, anyb, anyb, anyb],
        out_specs=(vm, vm, vm, vm, anyb, anyb, anyb, anyb),
        scratch_shapes=[
            V((half, width), bf16), V((half, width), bf16), V((half, width), bf16),
            V((2, lines, tok, width), bf16),
            V((lines, lines, 2, rows, tok), f32),
            V((lines, rows, cap, width), bf16),
            V((2, lines, 2, rows, cap, width), bf16),
            V((lines, m, half), bf16), V((lines, m, half), bf16), V((lines, m, half), bf16),
            V((2, lines, 2, rows, cap, width), bf16),
            V((lines, rows, cap, width), bf16),
            V((2, lines, rows, cap, width), bf16),
            V((2, lines, tok, width), bf16),
            V((2, lines + 1, tok, width), bf16),
            V((lines, rows, tok), f32),
            DMA((2, 2, lines)), DMA((2, lines)), DMA((2, lines)), DMA((lines,)),
            DMA((2, lines, rows)), DMA((2, lines, rows)),
            DMA((2, lines)), DMA((2, lines)), DMA((2, lines)), DMA((2, lines)),
            DMA((2, lines, rows)), DMA((2, lines, rows)),
            DMA((2, lines)), DMA((2, lines + 1)), DMA((lines,)), DMA((lines,)),
            DMA((3,)), DMA((5, lines)), DMA((rows,)), DMA((rows,)),
        ],
        compiler_params=pltpu.CompilerParams(
            collective_id=0, has_side_effects=True, vmem_limit_bytes=67043328
        ),
    )(scaled, gm, pos, rt, wgt, wut, wd)


def reduce_all(rows, cols, gain_at, terms, out, gains, one, two, mine, s1, r1, s2, r2, s3, r3):
    r = lax.axis_index("row")
    c = lax.axis_index("col")

    def rdma(src, dst, ss, rs, row, col):
        return pltpu.make_async_remote_copy(
            src_ref=src, dst_ref=dst, send_sem=ss, recv_sem=rs,
            device_id={"row": row, "col": col}, device_id_type=pl.DeviceIdType.MESH,
        )

    barrier = pltpu.get_barrier_semaphore()
    for o in range(1, rows):
        pl.semaphore_signal(barrier, inc=1, device_id={"row": (r + o) % rows, "col": c},
                            device_id_type=pl.DeviceIdType.MESH)
    for o in range(1, cols):
        pl.semaphore_signal(barrier, inc=1, device_id={"row": r, "col": (c + o) % cols},
                            device_id_type=pl.DeviceIdType.MESH)
    pl.semaphore_wait(barrier, rows + cols - 2)
    for o in range(1, rows):
        k = (r + o) % rows
        rdma(terms.at[k], one.at[r], s1.at[k], r1.at[r], k, c).start()
    total = terms[r]
    for o in range(1, rows):
        k = (r + o) % rows
        rdma(terms.at[k], one.at[k], s1.at[k], r1.at[k], k, c).wait()
        total = total + one[k]
    mine[...] = total
    two[c] = total
    for o in range(1, cols):
        k = (c + o) % cols
        rdma(mine, two.at[c], s2.at[k], r2.at[c], r, k).start()
    for o in range(1, cols):
        k = (c + o) % cols
        rdma(mine, two.at[k], s2.at[k], r2.at[k], r, k).wait()
    total = two[0]
    for k in range(1, cols):
        total = total + two[k]
    out[...] = total
    gains[r] = out[gain_at:gain_at + 8, :]
    for o in range(1, rows):
        k = (r + o) % rows
        rdma(gains.at[r], gains.at[r], s3.at[k], r3.at[r], k, c).start()
    for o in range(1, rows):
        k = (r + o) % rows
        rdma(gains.at[k], gains.at[k], s3.at[k], r3.at[k], k, c).wait()


def run_reduce(terms, rows, cols, gain_at):
    _, m, part = terms.shape
    DMA = pltpu.SemaphoreType.DMA
    vm = pl.BlockSpec(memory_space=pltpu.VMEM)
    return pl.pallas_call(
        functools.partial(reduce_all, rows, cols, gain_at),
        out_shape=(
            jax.ShapeDtypeStruct((m, part), f32),
            jax.ShapeDtypeStruct((rows, 8, part), f32),
        ),
        in_specs=[vm],
        out_specs=(vm, vm),
        scratch_shapes=[
            pltpu.VMEM((rows, m, part), f32), pltpu.VMEM((cols, m, part), f32),
            pltpu.VMEM((m, part), f32),
            DMA((rows,)), DMA((rows,)), DMA((cols,)), DMA((cols,)), DMA((rows,)), DMA((rows,)),
        ],
        compiler_params=pltpu.CompilerParams(collective_id=1, has_side_effects=True),
    )(terms)


def local(tokens, norm_gain, router_weight, expert_ids, w_gate, w_up, w_down, grad_mixed):
    tok, width = tokens.shape
    top = expert_ids.shape[1]
    experts = router_weight.shape[1]
    rows, lines = lax.axis_size("row"), lax.axis_size("col") // 2
    bound = 2 * ((2 * tok * top + 3 * experts - 1) // (3 * experts))
    cap = -(-bound // 16) * 16
    half = w_down.shape[1]
    block = 2 * lines * tok * width
    slot_block = 2 * lines * rows * cap * width
    needed = (6 * half * width + 4 * block + 2 * block // lines + 8 * slot_block
              + 12 * lines * rows * cap * half + 8 * block // lines)
    if needed > 15 * 2 ** 22:
        return wide_local(tokens, norm_gain, router_weight, expert_ids, w_gate, w_up, w_down,
                          grad_mixed)
    tokens_f = tokens.astype(f32)
    inverse = lax.rsqrt(jnp.mean(tokens_f * tokens_f, axis=1, keepdims=True) + epsilon)
    normed = tokens_f * inverse
    scaled = (normed * norm_gain).astype(bf16)
    expert_range = jnp.arange(experts, dtype=jnp.int32)
    chosen = jnp.any(expert_ids[:, :, None] == expert_range[None, None, :], axis=1)
    before = jnp.arange(tok)[:, None] < jnp.arange(tok)[None, :]
    rank = mm(chosen.astype(bf16), before.astype(bf16), TN)
    pos = jnp.where(chosen.T, rank, -1.0)
    acc, gg, meta, rt, x, hid, dg, du = run_exchange(
        scaled, grad_mixed, pos, router_weight.T, w_gate[0].T, w_up[0].T, w_down[0],
        rows, lines, cap,
    )
    by_expert = lambda v: v.transpose(1, 0, 2).reshape(experts, tok)
    scores = by_expert(meta[:, 1])
    grad_logits = (by_expert(gg) * scores * (1.0 - scores)).astype(bf16)
    router_t = rt.transpose(1, 0, 2).reshape(experts, width)
    grad_scaled = acc[1] + mm(grad_logits, router_t, TN)
    router_terms = mm(grad_logits, scaled)
    gain_terms = jnp.sum(grad_scaled * normed, axis=0)
    gain_at = -(-experts // 8) * 8
    terms = jnp.zeros((gain_at + 8, width), f32)
    terms = terms.at[:experts].set(router_terms).at[gain_at].set(gain_terms)
    terms = terms.reshape(gain_at + 8, rows, width // rows).transpose(1, 0, 2)
    summed, gains = run_reduce(terms, rows, 2 * lines, gain_at)
    grad_router = summed[:experts].T
    grad_gain = gains[:, 0].reshape(width)
    rows_in = x[0].reshape(-1, width)
    rows_grad = x[1].reshape(-1, width)
    half = hid.shape[-1]
    grad_wgate = mm(rows_in, dg.reshape(-1, half), TN).astype(bf16)
    grad_wup = mm(rows_in, du.reshape(-1, half), TN).astype(bf16)
    grad_wdown = mm(hid.reshape(-1, half), rows_grad, TN).astype(bf16)
    upstream = grad_mixed.astype(f32)
    mixed = (tokens_f + acc[0]).astype(bf16)
    grad_normed = grad_scaled * norm_gain
    grad_tokens = (
        upstream
        + inverse * (grad_normed - normed * jnp.mean(grad_normed * normed, axis=1, keepdims=True))
    ).astype(bf16)
    return (mixed, grad_tokens, grad_gain, grad_router,
            grad_wgate[None], grad_wup[None], grad_wdown[None])


def solution(mesh):
    both = ("row", "col")
    three = P(both, None, None)
    return jax.shard_map(
        local,
        mesh=mesh,
        in_specs=(P(both, None), P(), P("row", None), P(both, None), three, three, three,
                  P(both, None)),
        out_specs=(P(both, None), P(both, None), P(), P("row", None), three, three, three),
        check_vma=False,
    )
```
